32 devices in a mesh: row: 8 (over y, x, core), col: 4 (over z).
Axes of the slice: x: 2, y: 2, z: 4, core: 2. Of those that a mesh axis runs over, the one named last changes fastest.
Arguments:
- band_tiles: bfloat16 [8, 64, 256, 256], P('row', 'col'), may hold values from 0.0009994507 to 1
- band_cell: int32 [8, 64], P('row', 'col'), may hold values from 0 to 63, as said below
- band_count: int32 [8, 4], P('row', 'col'), may hold values from 1 to 16, as said below
- matrix_tiles: bfloat16 [8, 64, 256, 256], P('row', 'col'), may hold values from 7.390976e-05 to 0.07421875
- matrix_col: int32 [8, 64], P('row', 'col'), may hold values from 0 to 31
- matrix_live: int32 [8, 64], P('row', 'col'), may hold values 0 or 1
Outputs:
- reached: bfloat16 [4096, 32768], P('row', 'col')
- gained: float32 [], replicated
The draws below stay inside these ranges and needn't reach their ends.
Inputs may be any that keep to these rules, and one draw needn't show every extreme that they name: The band_cell values of one device's 16 slots are distinct. `band_count`: among the 4 devices of one index of row, the live slots with slot number 16 // 2 or more number at most 8 in all.
All inputs are finite; a program needn't handle non-finite values. No bound on the sum of `matrix_live` on one device may be relied on, other than what follows from the above.
Results may differ from the reference program's by a relative error of at most 0.001.
Values may be sent and summed in bfloat16 or wider, within the bound.
No kernel may reach another device: no remote copies, remote signals or barrier semaphores. Data moves between devices by JAX's collectives and lax.ppermute only.
A program may use at most 128 MiB of HBM per device.

```python
import math
import jax
import jax.numpy as jnp
from jax import lax

TILE = 256
TILES = 128
BR = 2
BS = 16
KR = 16
N_ROW = 8
N_COL = 4


def draw_band_cell(key, part):
    keys = jax.random.split(jax.random.fold_in(key, 11), N_ROW * N_COL)

    def one_device(single):
        return jax.random.permutation(single, BR * (TILES // N_COL))[:BS].astype(jnp.int32)
    cells = jax.vmap(one_device)(keys)
    return cells.reshape(N_ROW, N_COL * BS)


def draw_band_count(key, part):
    half = BS // 2
    light = jax.random.randint(jax.random.fold_in(key, 21), (N_ROW, N_COL), 1, half + 1)
    first = jax.random.randint(jax.random.fold_in(key, 22), (N_ROW,), half + 1, BS + 1)
    second = half + (BS - first)
    keys = jax.random.split(jax.random.fold_in(key, 23), N_ROW)

    def one_row(single):
        return jax.random.permutation(single, N_COL)[:2].astype(jnp.int32)
    heavy = jax.vmap(one_row)(keys)
    columns = jnp.arange(N_COL, dtype=jnp.int32)[None, :]
    counts = jnp.where(columns == heavy[:, 0:1], first[:, None], light)
    counts = jnp.where(columns == heavy[:, 1:2], second[:, None], counts)
    return counts.astype(jnp.int32)


def plant(entries, own_key, smallest, high):
    longest = entries.shape.index(max(entries.shape))
    spots = []
    for shift in (0, 1):
        where = [jax.random.randint(jax.random.fold_in(own_key, axis), (), 0, length) for axis, length in enumerate(entries.shape)]
        where[longest] = (where[longest] + shift) % entries.shape[longest]
        spots.append(tuple(where))
    return entries.at[spots[0]].set(smallest).at[spots[1]].set(high)


def steps_of(stream_key, extent, pieces, least, top_value):
    factor_of = 1.0
    for dim, parts in pieces:
        steps = jax.random.uniform(jax.random.fold_in(jax.random.fold_in(stream_key, 6), dim), (parts,), jnp.float32, least / len(pieces), top_value / len(pieces))
        factor_of = factor_of * jnp.repeat(jnp.exp(steps), extent[dim] // parts).reshape((-1,) + (1,) * (len(extent) - 1 - dim))
    return factor_of


def setup_inputs(seed: int = 0) -> dict:
    seeds = jax.random.split(jax.random.key(seed), 7)
    return {
        "band_tiles": jnp.clip(jnp.exp(math.log(1.0) - 6.9083047 * jax.random.uniform(seeds[0], (N_ROW, N_COL * BS, TILE, TILE), jnp.float32) ** steps_of(seeds[0], (N_ROW, N_COL * BS, TILE, TILE), ((0, 8), (1, 4)), -0.2, 0.2)), 0.0009994507, 1.0).astype(jnp.bfloat16),
        "band_cell": draw_band_cell(jax.random.fold_in(seeds[6], 71), 0),
        "band_count": draw_band_count(jax.random.fold_in(seeds[6], 71), 0),
        "matrix_tiles": jnp.clip(jnp.exp(math.log(0.07421875) - 6.911927 * jax.random.uniform(seeds[3], (N_ROW, N_COL * KR, TILE, TILE), jnp.float32) ** steps_of(seeds[3], (N_ROW, N_COL * KR, TILE, TILE), ((0, 8), (1, 4)), -0.2, 0.2)), 7.390975952148438e-05, 0.07421875).astype(jnp.bfloat16),
        "matrix_col": plant(jax.random.randint(seeds[4], (N_ROW, N_COL * KR), 0, TILES // N_COL), jax.random.fold_in(seeds[4], 1), 0, (TILES // N_COL) - 1).astype(jnp.int32),
        "matrix_live": plant((jax.random.randint(seeds[5], (N_ROW, N_COL * KR), 0, 3) < 2).astype(jnp.int32), jax.random.fold_in(seeds[5], 1), 0, 1),
    }


def reference(band_tiles, band_cell, band_count, matrix_tiles, matrix_col, matrix_live):
    tcols = TILES // N_COL
    krows = TILES // N_ROW
    slots = N_COL * BS
    places = BR * tcols
    tiles_col = matrix_tiles.reshape(N_ROW, N_COL, krows, TILE, TILE)
    index_col = matrix_col.reshape(N_ROW, N_COL, krows)
    live_col = matrix_live.reshape(N_ROW, N_COL, krows)
    slot = jnp.arange(slots, dtype=jnp.int32)
    source = slot // BS
    spots = jnp.arange(places, dtype=jnp.int32)

    def one_block(index):
        rindex = index // N_COL
        cindex = index % N_COL
        a_tiles = band_tiles[rindex]
        a_cell = band_cell[rindex]
        a_count = band_count[rindex]
        valid = (slot % BS) < a_count[source]
        k_glob = source * tcols + a_cell % tcols
        i_loc = a_cell // tcols
        b_tiles = tiles_col[:, cindex].reshape(TILES, TILE, TILE)
        b_index = index_col[:, cindex].reshape(TILES)
        b_live = live_col[:, cindex].reshape(TILES)
        picked = jnp.take(b_tiles, k_glob, axis=0)
        live = (jnp.take(b_live, k_glob) > 0) & valid
        position = i_loc * tcols + jnp.take(b_index, k_glob)
        product = jnp.einsum("axy,ayz->axz", a_tiles.astype(jnp.float32), picked.astype(jnp.float32), precision=lax.Precision.HIGHEST)
        weights = ((position[:, None] == spots[None, :]) & live[:, None]).astype(jnp.float32)
        summed = jnp.einsum("ap,axz->pxz", weights, product, precision=lax.Precision.HIGHEST)
        own_start = (cindex * BS).astype(jnp.int32)
        own_tiles = lax.dynamic_slice_in_dim(a_tiles, own_start, BS, 0)
        own_cell = lax.dynamic_slice_in_dim(a_cell, own_start, BS, 0)
        own_live = jnp.arange(BS, dtype=jnp.int32) < a_count[cindex]
        own_w = ((own_cell[:, None] == spots[None, :]) & own_live[:, None]).astype(jnp.float32)
        base = jnp.einsum("sp,sxz->pxz", own_w, own_tiles.astype(jnp.float32), precision=lax.Precision.HIGHEST)
        expanded = jnp.minimum(1.0, base + summed)
        block = expanded.reshape(BR, tcols, TILE, TILE).transpose(0, 2, 1, 3).reshape(BR * TILE, tcols * TILE)
        return block.astype(jnp.bfloat16), jnp.sum(expanded - base)

    blocks, sums = lax.map(one_block, jnp.arange(N_ROW * N_COL, dtype=jnp.int32))
    reached = blocks.reshape(N_ROW, N_COL, BR * TILE, tcols * TILE).transpose(0, 2, 1, 3).reshape(N_ROW * BR * TILE, N_COL * tcols * TILE)
    gained = jnp.sum(sums) / (TILE * TILE * N_ROW * N_COL * BR * tcols)
    return reached, gained
```

```python
import functools

import jax
import jax.numpy as jnp
from jax import lax
from jax.experimental import pallas as pl
from jax.experimental.pallas import tpu as pltpu
from jax.sharding import PartitionSpec as P

BR = 2
CHUNKS = 2


def pick(index, refs, fn, base=0):
    def rec(lo, hi):
        if hi - lo == 1:
            fn(refs[lo])
            return
        mid = (lo + hi) // 2
        pl.when(index < mid + base)(lambda: rec(lo, mid))
        pl.when(index >= mid + base)(lambda: rec(mid, hi))

    rec(0, len(refs))


class Layout:
    def __init__(self, n_row, n_col, slots, krows):
        self.n_row, self.n_col, self.slots, self.krows = n_row, n_col, slots, krows
        self.half = slots // 2
        self.chunk = self.half // CHUNKS
        self.tcols = n_row * krows // n_col
        self.places = BR * self.tcols
        self.most = n_col * self.half + self.half
        self.ahalf = krows // 2
        self.sets = n_row // 2
        steps = n_col - 1
        self.f_up = 1
        self.f_down = self.f_up + steps * CHUNKS
        self.f_spill = self.f_down + steps * CHUNKS
        self.f_refs = self.f_spill + steps * CHUNKS
        self.a_far = 2
        self.a_refs = 2 + 4 * (self.sets - 1)
        self.p_count = 0
        self.p_place = 8
        self.p_base = self.p_place + self.most
        self.p_start = self.p_base + self.most
        self.p_f = self.p_start + self.most + 1
        self.p_fi = self.p_f + self.most
        self.p_a = self.p_fi + self.most
        self.p_ai = self.p_a + self.most
        self.p_cover = self.p_ai + self.most
        self.p_size = -(-(self.p_cover + self.places) // 128) * 128


def plan_body(lay, ids, bands, mats, early, late, head, nxt, flag, own, pf, pfi, pa, pai):
    my_row, my_col = ids[0, 0], ids[0, 1]
    slots, half, n_col = lay.slots, lay.half, lay.n_col

    def clear(p, _):
        head[p] = -1
        flag[p] = 0
        own[p] = -1
        return 0

    lax.fori_loop(0, lay.places, clear, 0)

    def own_slot(s, _):
        own[bands[0, s]] = s
        return 0

    lax.fori_loop(0, bands[0, slots], own_slot, 0)

    def source(c, carry):
        total, spilled = carry
        row = lax.rem(my_col - c + n_col, n_col)
        count = bands[row, slots]
        mine = c == my_col
        step = jnp.maximum(jnp.abs(my_col - c), 1) - 1
        front = jnp.where(c < my_col, lay.f_up, lay.f_down) + step * CHUNKS
        spill_step = jnp.where(c < my_col, my_col, n_col - 1 - my_col) - 1
        back = lay.f_spill + spill_step * CHUNKS

        def slot(s, total):
            cell = bands[row, s]
            k = c * lay.tcols + lax.rem(cell, lay.tcols)
            i = lax.div(cell, lay.tcols)
            a_row = lax.div(k, lay.krows)
            a_slot = lax.rem(k, lay.krows)
            d = lax.bitwise_xor(a_row, my_row)
            far = lax.div(d, 2)
            core = lax.rem(d, 2)
            a_half = lax.div(a_slot, lay.ahalf)
            alive = mats[d, lay.krows + a_slot] > 0
            place = i * lay.tcols + mats[d, a_slot]
            in_front = s < half
            q = jnp.where(in_front, s, spilled + s - half)
            ref = jnp.where(in_front, front, back) + lax.div(q, lay.chunk)

            @pl.when(alive)
            def _():
                pf[total] = jnp.where(mine, 0, ref)
                pfi[total] = jnp.where(mine, s, lax.rem(q, lay.chunk))
                near = far == 0
                pa[total] = jnp.where(
                    near, core, lay.a_far + (core * 2 + a_half) * (lay.sets - 1) + far - 1
                )
                pai[total] = jnp.where(near, a_slot, lax.rem(a_slot, lay.ahalf))
                nxt[total] = head[place]
                head[place] = total

                @pl.when(jnp.logical_and(jnp.logical_not(mine), s >= half))
                def _():
                    flag[place] = 1

            return total + alive.astype(jnp.int32)

        total = lax.fori_loop(0, count, slot, total)
        return total, spilled + jnp.maximum(count - half, 0)

    lax.fori_loop(0, n_col, source, (jnp.int32(0), jnp.int32(0)))

    for which, out in ((0, early), (1, late)):

        def place_step(p, carry, which=which, out=out):
            n_place, n_prod = carry
            first = head[p]
            chosen = jnp.logical_and(first >= 0, flag[p] == which)
            out[0, lay.p_cover + p] = jnp.where(first >= 0, -2, own[p])

            @pl.when(chosen)
            def _():
                out[0, lay.p_place + n_place] = p
                out[0, lay.p_base + n_place] = own[p]
                out[0, lay.p_start + n_place] = n_prod

            def emit(state):
                at, n = state
                out[0, lay.p_f + n] = pf[at]
                out[0, lay.p_fi + n] = pfi[at]
                out[0, lay.p_a + n] = pa[at]
                out[0, lay.p_ai + n] = pai[at]
                return nxt[at], n + 1

            start = jnp.where(chosen, first, -1)
            _, n_prod = lax.while_loop(lambda state: state[0] >= 0, emit, (start, n_prod))
            return n_place + chosen.astype(jnp.int32), n_prod

        n_place, n_prod = lax.fori_loop(
            0, lay.places, place_step, (jnp.int32(0), jnp.int32(0))
        )
        out[0, lay.p_count] = n_place
        out[0, lay.p_count + 1] = n_prod
        out[0, lay.p_start + n_place] = n_prod


def expand_body(lay, tile, first, plan, *refs):
    nf, na = lay.f_refs, lay.a_refs
    if first:
        nf = lay.f_spill
    f_refs = refs[:nf]
    a_refs = refs[nf : nf + na]
    rest = refs[nf + na :]
    if first:
        out, gain = rest[:2]
        rest = rest[2:]
    else:
        gain_in, _, out, gain = rest[:4]
        rest = rest[4:]
    fbuf, abuf, bbuf, obuf, acc, part, sem_f, sem_a, sem_b, sem_o = rest[:10]
    n_place = plan[0, lay.p_count]
    n_prod = plan[0, lay.p_count + 1]
    band = f_refs[0]

    def spot(p):
        i = lax.div(p, lay.tcols)
        col = lax.rem(p, lay.tcols)
        return out.at[pl.ds(i * tile, tile), pl.ds(col * tile, tile)]

    def load(n, _):
        fi = plan[0, lay.p_fi + n]
        ai = plan[0, lay.p_ai + n]
        pick(
            plan[0, lay.p_f + n],
            f_refs,
            lambda ref: pltpu.make_async_copy(ref.at[fi], fbuf.at[n], sem_f.at[n]).start(),
        )
        pick(
            plan[0, lay.p_a + n],
            a_refs,
            lambda ref: pltpu.make_async_copy(ref.at[ai], abuf.at[n], sem_a.at[n]).start(),
        )
        return 0

    def load_base(t, _):
        b = plan[0, lay.p_base + t]

        @pl.when(b >= 0)
        def _():
            pltpu.make_async_copy(band.at[b], bbuf.at[t], sem_b.at[t]).start()

        @pl.when(b < 0)
        def _():
            bbuf[t] = jnp.zeros((tile, tile), jnp.bfloat16)

        return 0

    lax.fori_loop(0, n_prod, load, 0)
    lax.fori_loop(0, n_place, load_base, 0)

    if first:
        zero, sem_c = rest[10:12]
        zero[...] = jnp.zeros((tile, tile), jnp.bfloat16)

        def copy_of(p, b):
            return pltpu.make_async_copy(band.at[b], spot(p), sem_c.at[p])

        def clear_of(p):
            return pltpu.make_async_copy(zero, spot(p), sem_c.at[p])

        def cover(p, _):
            b = plan[0, lay.p_cover + p]
            pl.when(b >= 0)(lambda: copy_of(p, b).start())
            pl.when(b == -1)(lambda: clear_of(p).start())
            return 0

        lax.fori_loop(0, lay.places, cover, 0)

    part[...] = jnp.zeros((8, tile), jnp.float32)

    def place_step(t, _):
        b = plan[0, lay.p_base + t]
        start = plan[0, lay.p_start + t]
        stop = plan[0, lay.p_start + t + 1]

        @pl.when(b >= 0)
        def _():
            pltpu.make_async_copy(band.at[0], bbuf.at[t], sem_b.at[t]).wait()

        def product(n):
            pltpu.make_async_copy(band.at[0], fbuf.at[n], sem_f.at[n]).wait()
            pltpu.make_async_copy(band.at[0], abuf.at[n], sem_a.at[n]).wait()
            return jnp.dot(fbuf[n], abuf[n], preferred_element_type=jnp.float32)

        acc[...] = product(start)

        def more(n, _):
            acc[...] += product(n)
            return 0

        lax.fori_loop(start + 1, stop, more, 0)
        base = bbuf[t].astype(jnp.float32)
        grown = jnp.minimum(1.0, base + acc[...])
        part[...] += jnp.sum((grown - base).reshape(tile // 8, 8, tile), axis=0)
        obuf[t] = grown.astype(jnp.bfloat16)
        pltpu.make_async_copy(obuf.at[t], spot(plan[0, lay.p_place + t]), sem_o.at[t]).start()
        return 0

    lax.fori_loop(0, n_place, place_step, 0)
    total = jnp.sum(part[...])
    if not first:
        gain[...] = jnp.full(gain.shape, total, jnp.float32) + gain_in[...]
    else:
        gain[...] = jnp.full(gain.shape, total, jnp.float32)

    def drain(t, _):
        pltpu.make_async_copy(
            obuf.at[t], spot(plan[0, lay.p_place + t]), sem_o.at[t]
        ).wait()
        return 0

    lax.fori_loop(0, n_place, drain, 0)
    if first:

        def drain_cover(p, _):
            b = plan[0, lay.p_cover + p]
            pl.when(b >= 0)(lambda: copy_of(p, b).wait())
            pl.when(b == -1)(lambda: clear_of(p).wait())
            return 0

        lax.fori_loop(0, lay.places, drain_cover, 0)


def make_plan(lay, ids, bands, mats):
    smem = pl.BlockSpec(memory_space=pltpu.SMEM)
    shape = jax.ShapeDtypeStruct((1, lay.p_size), jnp.int32)
    scratch = [pltpu.SMEM((lay.most,), jnp.int32) for _ in range(5)]
    place = [pltpu.SMEM((lay.places,), jnp.int32) for _ in range(3)]
    order = [place[0], scratch[0], place[1], place[2], *scratch[1:]]
    return pl.pallas_call(
        functools.partial(plan_body, lay),
        in_specs=[smem] * 3,
        out_specs=[smem] * 2,
        out_shape=[shape] * 2,
        scratch_shapes=order,
        name="plan",
        cost_estimate=pl.CostEstimate(flops=20_000_000, bytes_accessed=8192, transcendentals=0),
    )(ids, bands, mats)


def expand(lay, tile, first, plan, f_bufs, a_bufs, gain_in=None, out_in=None):
    smem = pl.BlockSpec(memory_space=pltpu.SMEM)
    hbm = pl.BlockSpec(memory_space=pl.ANY)
    vmem = pl.BlockSpec(memory_space=pltpu.VMEM)
    ops = [plan, *f_bufs, *a_bufs]
    specs = [smem] + [hbm] * (len(ops) - 1)
    aliases = {}
    if not first:
        ops += [gain_in, out_in]
        specs += [vmem, hbm]
        aliases = {len(ops) - 1: 0}
    tiles = (lay.most, tile, tile)
    scratch = [
        pltpu.VMEM(tiles, jnp.bfloat16),
        pltpu.VMEM(tiles, jnp.bfloat16),
        pltpu.VMEM(tiles, jnp.bfloat16),
        pltpu.VMEM(tiles, jnp.bfloat16),
        pltpu.VMEM((tile, tile), jnp.float32),
        pltpu.VMEM((8, tile), jnp.float32),
        pltpu.SemaphoreType.DMA((lay.most,)),
        pltpu.SemaphoreType.DMA((lay.most,)),
        pltpu.SemaphoreType.DMA((lay.most,)),
        pltpu.SemaphoreType.DMA((lay.most,)),
    ]
    if first:
        scratch += [
            pltpu.VMEM((tile, tile), jnp.bfloat16),
            pltpu.SemaphoreType.DMA((lay.places,)),
        ]
    out_shape = [
        jax.ShapeDtypeStruct((BR * tile, lay.tcols * tile), jnp.bfloat16),
        jax.ShapeDtypeStruct((8, 128), jnp.float32),
    ]
    flops = 2 * tile**3 * lay.most
    return pl.pallas_call(
        functools.partial(expand_body, lay, tile, first),
        in_specs=specs,
        out_specs=[hbm, vmem],
        out_shape=out_shape,
        scratch_shapes=scratch,
        input_output_aliases=aliases,
        name="expand_early" if first else "expand_late",
        cost_estimate=pl.CostEstimate(
            flops=flops, bytes_accessed=24 * lay.most * tile * tile, transcendentals=0
        ),
    )(*ops)


def on_device(band_tiles, band_cell, band_count, matrix_tiles, matrix_col, matrix_live):
    n_row, n_col = lax.axis_size("row"), lax.axis_size("col")
    slots, krows, tile = band_tiles.shape[1], matrix_tiles.shape[1], band_tiles.shape[-1]
    lay = Layout(n_row, n_col, slots, krows)
    half, chunk = lay.half, lay.chunk
    my_row, my_col = lax.axis_index("row"), lax.axis_index("col")
    band, mat = band_tiles[0], matrix_tiles[0]
    up = [(i, i + 1) for i in range(n_col - 1)]
    down = [(i + 1, i) for i in range(n_col - 1)]

    def hop(x, bit):
        return lax.ppermute(x, "row", [(i, i ^ bit) for i in range(n_row)])

    def turn(x, by):
        return lax.ppermute(x, "col", [(i, (i + by) % n_col) for i in range(n_col)])

    band_meta = jnp.concatenate([band_cell, band_count], axis=1)
    mat_meta = jnp.concatenate([matrix_col, matrix_live], axis=1)
    bands = jnp.concatenate([band_meta] + [turn(band_meta, d) for d in range(1, n_col)], axis=0)
    mats = jnp.concatenate([mat_meta] + [hop(mat_meta, d) for d in range(1, n_row)], axis=0)
    ids = jnp.stack([my_row, my_col]).astype(jnp.int32)[None]

    ups, downs = [], []
    u = d = [band[c * chunk : (c + 1) * chunk] for c in range(CHUNKS)]
    for step in range(n_col - 1):
        u = [lax.ppermute(x, "col", up[step:]) for x in u]
        d = [lax.ppermute(x, "col", down[: n_col - 1 - step]) for x in d]
        ups += u
        downs += d

    bits = [1 << b for b in range(1, n_row.bit_length() - 1)]
    near = [mat, hop(mat, 1)]
    far = []
    for h, order in enumerate((bits, bits[::-1])):
        got = {0: mat[h * lay.ahalf : (h + 1) * lay.ahalf]}
        for bit in order:
            got.update({key | bit: hop(x, bit) for key, x in list(got.items())})
        far += [got[2 * m] for m in range(1, lay.sets)]
    a_bufs = near + far + [hop(x, 1) for x in far]

    source = lax.rem(my_col - jnp.arange(n_col) + n_col, n_col)
    spill = jnp.maximum(bands[:, slots] - half, 0)
    before = jnp.sum(jnp.where(source < my_col, spill, 0))
    q = jnp.arange(half, dtype=jnp.int32)
    held = (q >= before) & (q < before + spill[0])
    packed = jnp.take(band, jnp.clip(half + q - before, 0, slots - 1), axis=0)
    packed = [packed[c * chunk : (c + 1) * chunk] for c in range(CHUNKS)]
    held = [held[c * chunk : (c + 1) * chunk, None, None] for c in range(CHUNKS)]
    spills = []
    got = packed
    for step in range(1, n_col):
        pairs = [(step - 1, step), (n_col - step, n_col - step - 1)]
        got = [lax.ppermute(x, "col", pairs) for x in got]
        spills += got
        got = [jnp.where(h, p, x) for h, p, x in zip(held, packed, got)]

    early, late = make_plan(lay, ids, bands, mats)
    f_bufs = [band, *ups, *downs]
    out, gain = expand(lay, tile, True, early, f_bufs, a_bufs)
    out, gain = expand(lay, tile, False, late, f_bufs + spills, a_bufs, gain, out)

    gain = gain[:1, :1]
    for b in range(n_row.bit_length() - 1):
        gain = gain + hop(gain, 1 << b)
    for b in range(n_col.bit_length() - 1):
        gain = gain + lax.ppermute(gain, "col", [(i, i ^ (1 << b)) for i in range(n_col)])
    gained = gain[0, 0] / (tile * tile * n_row * n_col * lay.places)
    return out, gained


def solution(mesh):
    in_specs = (
        P("row", "col", None, None),
        P("row", "col"),
        P("row", "col"),
        P("row", "col", None, None),
        P("row", "col"),
        P("row", "col"),
    )
    out_specs = (P("row", "col"), P())
    return jax.shard_map(
        on_device, mesh=mesh, in_specs=in_specs, out_specs=out_specs, check_vma=False
    )
```
